128 devices in a mesh: res: 4 (over x_hi, core), blk: 32 (over x_lo, y, z).
Axes of the slice: x: 4 (x_hi: 2, x_lo: 2; x = x_hi * 2 + x_lo), y: 4, z: 4, core: 2. Of those that a mesh axis runs over, the one named last changes fastest.
Arguments:
- modes: float32 [2, 8, 4194304], P(None, 'res', 'blk'), may hold values from -0.078125 to 0.078125
Outputs:
- product_modes: float32 [2, 8, 4194304], P(None, 'res', 'blk')
The draws below stay inside these ranges and needn't reach their ends.
All inputs are finite; a program needn't handle non-finite values.
Results may differ from the reference program's by a relative error of at most 0.000098.
Values sent between devices are 32-bit elements; how exact they have to be, the bound alone decides.
A program may use at most 128 MiB of HBM per device.

```python
import jax
import jax.numpy as jnp

MODES = 33554432
EIGHTH = 4194304
PADDED = 50331648


def block_levels(key, extent, cuts, smallest, largest):
    gain, own = 1.0, jax.random.fold_in(key, 6)
    for dim, blocks in cuts:
        heights = jnp.exp(jax.random.uniform(jax.random.fold_in(own, dim), (blocks,), jnp.float32, smallest / len(cuts), largest / len(cuts)))
        gain = gain * jnp.repeat(heights, extent[dim] // blocks).reshape([-1 if axis == dim else 1 for axis in range(len(extent))])
    return gain


def gaussian(own_key, dims, scale, most, shards=(), dtype=jnp.bfloat16):
    loudness = block_levels(own_key, dims, shards, -0.22, 0.18) if shards else 1.0
    values = jax.random.normal(own_key, dims, jnp.float32) * scale * loudness
    return jnp.minimum(jnp.maximum(values, -most), most).astype(dtype)


def setup_inputs(seed: int = 0) -> dict:
    key_of = jax.random.split(jax.random.key(seed), 2)
    modes = gaussian(key_of[0], (2, 8, EIGHTH), (MODES ** -0.25), 0.078125, ((1, 4), (2, 32)), jnp.float32)
    return {"modes": modes}


def reference(modes):
    series = (modes[0] + 1j * modes[1]).reshape(MODES)
    padded = jnp.pad(series, (0, PADDED - MODES))
    physical = jnp.fft.ifft(padded) * PADDED
    spectrum = jnp.fft.fft(physical * physical) / PADDED
    kept = spectrum[MODES // 2: MODES // 2 + MODES]
    result = jnp.stack([jnp.real(kept), jnp.imag(kept)]).reshape(2, 8, EIGHTH)
    return result.astype(jnp.float32)
```

```python
import math

import jax
import jax.numpy as jnp
import numpy as np
from jax import lax
from jax.experimental import pallas as pl
from jax.experimental.pallas import tpu as pltpu
from jax.sharding import PartitionSpec as P

F32, BF16 = jnp.float32, jnp.bfloat16
DEVICES = 128
PADDED = 50331648
LOCAL = 131072
STEP = 37
MESH = pl.DeviceIdType.MESH
HALF_ROOT3 = math.sqrt(3.0) / 2.0
ROOT_HALF = math.sqrt(0.5)


def real_block(w):
    return np.block([[w.real, -w.imag], [w.imag, w.real]])


def high_low(w):
    high = np.asarray(w, np.float32).astype(jnp.bfloat16)
    low = (w - high.astype(np.float64)).astype(np.float32).astype(jnp.bfloat16)
    return np.stack([high, low])


def root(turns):
    return np.exp(2j * np.pi * (turns % 1.0))


def tables():
    n = np.arange(128)
    kl = np.array([(u // 32) * 64 + e * 32 + u % 32 for e in range(2) for u in range(64)])
    first, last = [], []
    for s in range(3):
        w = root(np.outer(n, kl) / 128.0) * root(kl * s / 384.0)[None, :]
        first.append(high_low(real_block(w)))
        last.append(high_low(real_block(w).T / PADDED))
    f = real_block(root(np.outer(n, n) / 128.0))
    turn = [root(np.outer(3 * n + s, n) / PADDED) for s in range(3)]
    turn.append(root(np.outer(n, n) / 16384.0))
    columns = np.zeros((128, 128), np.complex128)
    columns[:, :8] = root(np.outer(n, np.arange(8)) / 1024.0)
    turn.append(columns)
    rows = np.zeros((128, 128), np.complex128)
    rows[:8] = root(np.outer(np.arange(8), n) / LOCAL)
    turn.append(rows)
    turn = np.stack([np.stack([t.real, t.imag]) for t in turn]).astype(np.float32)
    return (
        np.stack(first),
        np.stack(last),
        np.stack([high_low(f), high_low(f.T)]),
        turn,
    )


def split(x):
    high = x.astype(BF16)
    return high, (x - high.astype(F32)).astype(BF16)


def dot(a, b):
    return jnp.dot(a, b, preferred_element_type=F32)


def left(w_high, w_low, x):
    high, low = split(x)
    return dot(w_high, high) + dot(w_high, low) + dot(w_low, high)


def right(x, w_high, w_low):
    high, low = split(x)
    return dot(high, w_high) + dot(low, w_high) + dot(high, w_low)


def times(a, b):
    return a[0] * b[0] - a[1] * b[1], a[0] * b[1] + a[1] * b[0]


def times_conj(a, b):
    return a[0] * b[0] + a[1] * b[1], a[1] * b[0] - a[0] * b[1]


def add(a, b):
    return a[0] + b[0], a[1] + b[1]


def sub(a, b):
    return a[0] - b[0], a[1] - b[1]


def quarter(a, sign):
    return (-a[1], a[0]) if sign > 0 else (a[1], -a[0])


def eighth(a, sign):
    if sign > 0:
        return (a[0] - a[1]) * ROOT_HALF, (a[0] + a[1]) * ROOT_HALF
    return (a[0] + a[1]) * ROOT_HALF, (a[1] - a[0]) * ROOT_HALF


def four(a, b, c, d, sign):
    p, q, r, t = add(a, c), sub(a, c), add(b, d), quarter(sub(b, d), sign)
    return add(p, r), add(q, t), sub(p, r), sub(q, t)


def eight(v, sign):
    even = four(v[0], v[2], v[4], v[6], sign)
    odd = four(v[1], v[3], v[5], v[7], sign)
    odd = (
        odd[0],
        eighth(odd[1], sign),
        quarter(odd[2], sign),
        quarter(eighth(odd[3], sign), sign),
    )
    return [add(e, o) for e, o in zip(even, odd)] + [sub(e, o) for e, o in zip(even, odd)]


def kernel(
    x_ref, first_hbm, last_hbm, fg_hbm, turn_hbm, o_ref,
    first, last, fg, turn, got1, put2, got2, put3, got3, put4,
    outer_turn, column_turn, inner_turn, high, low, back, held,
    const_sem, own_sem, send1, recv1, send2, recv2, send3, recv3, send4, recv4,
):
    r, b = lax.axis_index("res"), lax.axis_index("blk")
    me = r * 32 + b

    constants = [
        pltpu.make_async_copy(src, dst, const_sem.at[i])
        for i, (src, dst) in enumerate(
            ((first_hbm, first), (last_hbm, last), (fg_hbm, fg), (turn_hbm, turn))
        )
    ]
    for copy in constants:
        copy.start()
    own_in = pltpu.make_async_copy(x_ref.at[:, me], got1.at[:, :, me], own_sem.at[0])
    own_in.start()

    def everyone(body):
        def step(i, carry):
            to = (me + i * STEP) % DEVICES
            body(to, {"res": to // 32, "blk": to % 32})
            return carry

        lax.fori_loop(1, DEVICES, step, 0)

    barrier = pltpu.get_barrier_semaphore()
    everyone(
        lambda to, device: pl.semaphore_signal(
            barrier, inc=1, device_id=device, device_id_type=MESH
        )
    )
    pl.semaphore_wait(barrier, DEVICES - 1)

    def remote(src, dst, send, recv, device):
        return pltpu.make_async_remote_copy(
            src_ref=src,
            dst_ref=dst,
            send_sem=send,
            recv_sem=recv,
            device_id=device,
            device_id_type=MESH,
        )

    def here(src, dst, send, recv):
        return remote(src, dst, send, recv, {"res": r, "blk": b})

    everyone(
        lambda to, device: remote(
            x_ref.at[:, to], got1.at[:, :, me], send1, recv1, device
        ).start()
    )

    for copy in constants:
        copy.wait()

    n1 = lax.broadcasted_iota(jnp.int32, (128, 128), 0)
    lane = lax.broadcasted_iota(jnp.int32, (128, 128), 1)
    angle = ((8 * me + lane % 8) * (3 * n1 + lane // 8)).astype(F32) * (
        2.0 * math.pi * 128.0 / PADDED
    )
    cosine, sine = jnp.cos(angle), jnp.sin(angle)
    for s in range(3):
        for s8 in range(8):
            at = 8 * s + s8
            column = (
                jnp.broadcast_to(cosine[:, at : at + 1], (128, 128)),
                jnp.broadcast_to(sine[:, at : at + 1], (128, 128)),
            )
            re, im = times(column, (turn[s, 0], turn[s, 1]))
            outer_turn[s, s8, 0] = re
            outer_turn[s, s8, 1] = im
    for a in range(8):
        for part in range(2):
            column_turn[a, part] = jnp.broadcast_to(turn[4, part, :, a : a + 1], (128, 128))
        row = (
            jnp.broadcast_to(turn[5, 0, a : a + 1, :], (128, 128)),
            jnp.broadcast_to(turn[5, 1, a : a + 1, :], (128, 128)),
        )
        re, im = times(row, (turn[3, 0], turn[3, 1]))
        inner_turn[a, 0] = re
        inner_turn[a, 1] = im

    own_in.wait()
    some = pl.ds(0, DEVICES - 1)
    here(x_ref.at[:, some], got1.at[:, :, some], send1, recv1).wait_recv()

    rows1 = got1.reshape(2 * 2 * 128 * 8, 128)
    rows2 = put2.reshape(3 * 2 * 128 * 8, 128)
    rows3 = got3.reshape(3 * 2 * 128 * 8, 128)
    rows4 = put4.reshape(2 * 2 * 128 * 8, 128)

    def outer_forward(s):
        cr = (1.0, -0.5, -0.5)[s]
        ci = (0.0, HALF_ROOT3, -HALF_ROOT3)[s]

        def body(h, carry):
            columns = []
            for j in range(2):
                def block(part, upper):
                    at = ((part * 2 + h // 2) * 128 + upper * 64) * 8 + ((h % 2) * 2 + j) * 2
                    return jnp.concatenate(
                        [rows1[pl.ds(at + e, 64, stride=8), :] for e in range(2)], axis=0
                    )

                x0, x1 = (block(0, 0), block(1, 0)), (block(0, 1), block(1, 1))
                if s == 0:
                    y = add(x0, x1)
                else:
                    y = (
                        x0[0] + cr * x1[0] - ci * x1[1],
                        x0[1] + cr * x1[1] + ci * x1[0],
                    )
                columns.append(jnp.concatenate(y, axis=0))
            out = left(first[s, 0], first[s, 1], jnp.concatenate(columns, axis=1))
            for j in range(2):
                s8 = 2 * h + j
                part = (out[:128, 128 * j : 128 * j + 128], out[128:, 128 * j : 128 * j + 128])
                re, im = times(part, (outer_turn[s, s8, 0], outer_turn[s, s8, 1]))
                rows2[pl.ds((s * 2) * 1024 + s8, 128, stride=8), :] = re
                rows2[pl.ds((s * 2 + 1) * 1024 + s8, 128, stride=8), :] = im
            return carry

        lax.fori_loop(0, 4, body, 0)

    mine = pl.ds(pl.multiple_of(8 * me, 8), 8)
    for s in range(3):
        outer_forward(s)
        got2[s, :, mine, :] = put2[s, :, me]
        everyone(
            lambda to, device: remote(
                put2.at[s, :, to], got2.at[s, :, mine, :], send2.at[s], recv2.at[s], device
            ).start()
        )

    def inner(s):
        def open_eight(i, carry):
            at = pl.multiple_of(16 * i, 16)
            v = [
                (got2[s, 0, pl.ds(128 * a + at, 16), :], got2[s, 1, pl.ds(128 * a + at, 16), :])
                for a in range(8)
            ]
            for a, y in enumerate(eight(v, 1)):
                if a:
                    y = times(y, (column_turn[a, 0, pl.ds(at, 16), :], column_turn[a, 1, pl.ds(at, 16), :]))
                for part in range(2):
                    up, down = split(y[part])
                    high[a, pl.ds(128 * part + at, 16), :] = up
                    low[a, pl.ds(128 * part + at, 16), :] = down
            return carry

        lax.fori_loop(0, 8, open_eight, 0)

        def middle(h, carry):
            pair = (2 * h, 2 * h + 1)
            up = jnp.concatenate([high[a] for a in pair], axis=1)
            down = jnp.concatenate([low[a] for a in pair], axis=1)
            out = dot(fg[0, 0], up) + dot(fg[0, 0], down) + dot(fg[0, 1], up)
            lines = []
            for j, a in enumerate(pair):
                y = (out[:128, 128 * j : 128 * j + 128], out[128:, 128 * j : 128 * j + 128])
                lines.append(jnp.concatenate(times(y, (inner_turn[a, 0], inner_turn[a, 1])), axis=1))
            v = right(jnp.concatenate(lines, axis=0), fg[1, 0], fg[1, 1])
            re, im = v[:, :128], v[:, 128:]
            squared = jnp.concatenate([(re + im) * (re - im), 2.0 * re * im], axis=1)
            v = right(squared, fg[0, 0], fg[0, 1])
            columns = []
            for j, a in enumerate(pair):
                y = (v[128 * j : 128 * j + 128, :128], v[128 * j : 128 * j + 128, 128:])
                columns.append(
                    jnp.concatenate(times_conj(y, (inner_turn[a, 0], inner_turn[a, 1])), axis=0)
                )
            out = left(fg[1, 0], fg[1, 1], jnp.concatenate(columns, axis=1))
            for j, a in enumerate(pair):
                y = (out[:128, 128 * j : 128 * j + 128], out[128:, 128 * j : 128 * j + 128])
                re, im = times_conj(y, (column_turn[a, 0], column_turn[a, 1]))
                back[a, 0] = re
                back[a, 1] = im
            return carry

        lax.fori_loop(0, 4, middle, 0)

        def close_eight(i, carry):
            at = pl.multiple_of(16 * i, 16)
            v = [(back[a, 0, pl.ds(at, 16), :], back[a, 1, pl.ds(at, 16), :]) for a in range(8)]
            for a, y in enumerate(eight(v, -1)):
                for part in range(2):
                    put3[s, part, pl.ds(128 * a + at, 16), :] = y[part]
            return carry

        lax.fori_loop(0, 8, close_eight, 0)

    most = pl.ds(0, 8 * (DEVICES - 1))
    for s in range(3):
        here(put3.at[s, :, most, :], got2.at[s, :, most, :], send2.at[s], recv2.at[s]).wait_recv()
        inner(s)
        got3[s, :, me] = put3[s, :, mine, :]
        everyone(
            lambda to, device: remote(
                put3.at[s, :, pl.ds(pl.multiple_of(8 * to, 8), 8), :],
                got3.at[s, :, me],
                send3.at[s],
                recv3.at[s],
                device,
            ).start()
        )

    def outer_backward(s, h):
        columns = []
        for j in range(2):
            s8 = 2 * h + j
            z = (
                rows3[pl.ds((s * 2) * 1024 + s8, 128, stride=8), :],
                rows3[pl.ds((s * 2 + 1) * 1024 + s8, 128, stride=8), :],
            )
            z = times_conj(z, (outer_turn[s, s8, 0], outer_turn[s, s8, 1]))
            columns.append(jnp.concatenate(z, axis=0))
        return left(last[s, 0], last[s, 1], jnp.concatenate(columns, axis=1))

    def wait3(s):
        here(
            put2.at[s, :, some], got3.at[s, :, some], send3.at[s], recv3.at[s]
        ).wait_recv()

    for s in range(2):
        wait3(s)

        def keep(h, carry):
            held[s, h] = outer_backward(s, h)
            return carry

        lax.fori_loop(0, 4, keep, 0)

    wait3(2)
    own_out = []
    for t in range(2):
        def finish(g, carry):
            h = 2 * t + g
            y0, y1, y2 = held[0, h], held[1, h], outer_backward(2, h)
            u, v = y1 + y2, HALF_ROOT3 * (y1 - y2)
            y = y0 - 0.5 * u
            re, im, vr, vi = y[:128], y[128:], v[:128], v[128:]
            for upper, out in enumerate(((re + vi, im - vr), (re - vi, im + vr))):
                for part in range(2):
                    for j in range(2):
                        for e in range(2):
                            at = ((part * 2 + t) * 128 + upper * 64) * 8 + (g * 2 + j) * 2 + e
                            rows4[pl.ds(at, 64, stride=8), :] = out[part][
                                64 * e : 64 * e + 64, 128 * j : 128 * j + 128
                            ]
            return carry

        lax.fori_loop(0, 2, finish, 0)
        own = pltpu.make_async_copy(put4.at[:, t, me], o_ref.at[:, me, t], own_sem.at[1 + t])
        own.start()
        own_out.append(own)
        everyone(
            lambda to, device: remote(
                put4.at[:, t, to], o_ref.at[:, me, t], send4.at[t], recv4.at[t], device
            ).start()
        )

    for own in own_out:
        own.wait()
    here(x_ref.at[:, some], got1.at[:, :, some], send1, recv1).wait_send()
    for s in range(3):
        here(put2.at[s, :, some], got3.at[s, :, some], send2.at[s], recv3.at[s]).wait_send()
        here(put2.at[s, :, some], got3.at[s, :, some], send3.at[s], recv3.at[s]).wait_send()
    for t in range(2):
        here(put4.at[:, t, some], o_ref.at[:, some, t], send4.at[t], recv4.at[t]).wait()


def solution(mesh):
    constants = tables()

    def on_device(modes):
        x = modes.reshape(2, 2, 1024, 128).transpose(0, 2, 1, 3).reshape(2, 128, 2, 8, 128)
        anywhere = pl.BlockSpec(memory_space=pl.ANY)
        dma = pltpu.SemaphoreType.DMA
        out = pl.pallas_call(
            kernel,
            out_shape=jax.ShapeDtypeStruct((2, 128, 2, 8, 128), F32),
            in_specs=[anywhere] * 5,
            out_specs=anywhere,
            scratch_shapes=[
                pltpu.VMEM((3, 2, 256, 256), BF16),
                pltpu.VMEM((3, 2, 256, 256), BF16),
                pltpu.VMEM((2, 2, 256, 256), BF16),
                pltpu.VMEM((6, 2, 128, 128), F32),
                pltpu.VMEM((2, 2, 128, 8, 128), F32),
                pltpu.VMEM((3, 2, 128, 8, 128), F32),
                pltpu.VMEM((3, 2, 1024, 128), F32),
                pltpu.VMEM((3, 2, 1024, 128), F32),
                pltpu.VMEM((3, 2, 128, 8, 128), F32),
                pltpu.VMEM((2, 2, 128, 8, 128), F32),
                pltpu.VMEM((3, 8, 2, 128, 128), F32),
                pltpu.VMEM((8, 2, 128, 128), F32),
                pltpu.VMEM((8, 2, 128, 128), F32),
                pltpu.VMEM((8, 256, 128), BF16),
                pltpu.VMEM((8, 256, 128), BF16),
                pltpu.VMEM((8, 2, 128, 128), F32),
                pltpu.VMEM((2, 4, 256, 256), F32),
                dma((4,)),
                dma((3,)),
                dma,
                dma,
                dma((3,)),
                dma((3,)),
                dma((3,)),
                dma((3,)),
                dma((2,)),
                dma((2,)),
            ],
            compiler_params=pltpu.CompilerParams(
                collective_id=0, has_side_effects=True, vmem_limit_bytes=56 * 2**20
            ),
        )(x, *(jnp.asarray(c) for c in constants))
        return out.reshape(2, 1024, 2, 128).transpose(0, 2, 1, 3).reshape(2, 2, LOCAL)

    spec = P(None, "res", "blk")
    return jax.shard_map(on_device, mesh=mesh, in_specs=(spec,), out_specs=spec, check_vma=False)
```

```python
import math

import jax
import jax.numpy as jnp
import numpy as np
from jax import lax
from jax.experimental import pallas as pl
from jax.experimental.pallas import tpu as pltpu
from jax.sharding import PartitionSpec as P

F32, BF16 = jnp.float32, jnp.bfloat16
DEVICES = 128
PADDED = 50331648
LOCAL = 131072
STEP = 37
MESH = pl.DeviceIdType.MESH
HALF_ROOT3 = math.sqrt(3.0) / 2.0
ROOT_HALF = math.sqrt(0.5)


def real_block(w):
    return np.block([[w.real, -w.imag], [w.imag, w.real]])


def high_low(w):
    high = np.asarray(w, np.float32).astype(jnp.bfloat16)
    low = (w - high.astype(np.float64)).astype(np.float32).astype(jnp.bfloat16)
    return np.stack([high, low])


def root(turns):
    return np.exp(2j * np.pi * (turns % 1.0))


def tables():
    n = np.arange(128)
    kl = np.array([(u // 32) * 64 + e * 32 + u % 32 for e in range(2) for u in range(64)])
    first, last = [], []
    for s in range(3):
        w = root(np.outer(n, kl) / 128.0) * root(kl * s / 384.0)[None, :]
        first.append(high_low(real_block(w)))
        last.append(high_low(real_block(w).T / PADDED))
    mixed = (n % 64) // 4 * 8 + n // 64 * 4 + n % 4
    f = real_block(root(np.outer(n, mixed) / 128.0))
    turn = [root(np.outer(3 * n + s, n) / PADDED) for s in range(3)]
    turn.append(root(np.outer(n, n) / 16384.0))
    columns = np.zeros((128, 128), np.complex128)
    columns[:, :8] = root(np.outer(mixed, np.arange(8)) / 1024.0)
    turn.append(columns)
    rows = np.zeros((128, 128), np.complex128)
    rows[:8] = root(np.outer(np.arange(8), n) / LOCAL)
    turn.append(rows)
    turn = np.stack([np.stack([t.real, t.imag]) for t in turn]).astype(np.float32)
    return (
        np.stack(first),
        np.stack(last),
        np.stack([high_low(f), high_low(f.T)]),
        turn,
    )


def split(x):
    high = x.astype(BF16)
    return high, (x - high.astype(F32)).astype(BF16)


def dot(a, b):
    return jnp.dot(a, b, preferred_element_type=F32)


def left(w_high, w_low, x):
    high, low = split(x)
    return dot(w_high, high) + dot(w_high, low) + dot(w_low, high)


def right(x, w_high, w_low):
    high, low = split(x)
    return dot(high, w_high) + dot(low, w_high) + dot(high, w_low)


def times(a, b):
    return a[0] * b[0] - a[1] * b[1], a[0] * b[1] + a[1] * b[0]


def times_conj(a, b):
    return a[0] * b[0] + a[1] * b[1], a[1] * b[0] - a[0] * b[1]


def add(a, b):
    return a[0] + b[0], a[1] + b[1]


def sub(a, b):
    return a[0] - b[0], a[1] - b[1]


def quarter(a, sign):
    return (-a[1], a[0]) if sign > 0 else (a[1], -a[0])


def eighth(a, sign):
    if sign > 0:
        return (a[0] - a[1]) * ROOT_HALF, (a[0] + a[1]) * ROOT_HALF
    return (a[0] + a[1]) * ROOT_HALF, (a[1] - a[0]) * ROOT_HALF


def four(a, b, c, d, sign):
    p, q, r, t = add(a, c), sub(a, c), add(b, d), quarter(sub(b, d), sign)
    return add(p, r), add(q, t), sub(p, r), sub(q, t)


def eight(v, sign):
    even = four(v[0], v[2], v[4], v[6], sign)
    odd = four(v[1], v[3], v[5], v[7], sign)
    odd = (
        odd[0],
        eighth(odd[1], sign),
        quarter(odd[2], sign),
        quarter(eighth(odd[3], sign), sign),
    )
    return [add(e, o) for e, o in zip(even, odd)] + [sub(e, o) for e, o in zip(even, odd)]


def kernel(
    x_ref, first_hbm, last_hbm, fg_hbm, turn_hbm, o_ref,
    first, last, fg, turn, got1, put2, got2, put3, got3, put4,
    outer_turn, column_turn, inner_turn, high, low, back, held,
    near_sem, const_sem, own_sem, send1, recv1, send2, recv2, send3, recv3, send4, recv4,
):
    r, b = lax.axis_index("res"), lax.axis_index("blk")
    me = r * 32 + b

    constants = [
        pltpu.make_async_copy(src, dst, const_sem.at[i])
        for i, (src, dst) in enumerate(
            ((first_hbm, first), (last_hbm, last), (fg_hbm, fg), (turn_hbm, turn))
        )
    ]
    for copy in constants:
        copy.start()
    own_in = pltpu.make_async_copy(x_ref.at[:, me], got1.at[:, :, me], own_sem.at[0])
    own_in.start()

    def remote(src, dst, send, recv, device):
        return pltpu.make_async_remote_copy(
            src_ref=src,
            dst_ref=dst,
            send_sem=send,
            recv_sem=recv,
            device_id=device,
            device_id_type=MESH,
        )

    def here(src, dst, send, recv):
        return remote(src, dst, send, recv, {"res": r, "blk": b})

    def everyone(body):
        def step(i, carry):
            to = (me + i * STEP) % DEVICES
            body(to, {"res": to // 32, "blk": to % 32})
            return carry

        lax.fori_loop(1, DEVICES, step, 0)

    at_x, at_y, at_z, at_core = r // 2 * 2 + b // 16, b // 4 % 4, b % 4, r % 2

    def away(body, x=0, y=0, z=0, core=0):
        to_x = (at_x + x) % 4
        res = to_x // 2 * 2 + (at_core + core) % 2
        blk = to_x % 2 * 16 + (at_y + y) % 4 * 4 + (at_z + z) % 4
        body(res * 32 + blk, {"res": res, "blk": blk})

    def loop(count, body):
        def step(i, carry):
            body(i)
            return carry

        lax.fori_loop(0, count, step, 0)

    def one(body):
        def step(i):
            away(body, x=1 + i)
            away(body, y=1 + i)
            away(body, z=1 + i)

        loop(3, step)
        away(body, core=1)

    def two(body):
        def step(i):
            p, q = 1 + i % 3, 1 + i // 3
            away(body, x=p, y=q)
            away(body, y=p, z=q)
            away(body, z=p, x=q)

        loop(9, step)

        def over(i):
            away(body, x=1 + i, core=1)
            away(body, y=1 + i, core=1)
            away(body, z=1 + i, core=1)

        loop(3, over)

    def three(body):
        def step(i):
            p, q = 1 + i % 3, 1 + i // 3
            for u in range(3):
                away(body, x=p, y=q, z=1 + u)
            away(body, x=p, y=q, core=1)
            away(body, y=p, z=q, core=1)
            away(body, z=p, x=q, core=1)

        loop(9, step)

    def four_apart(body):
        def step(i):
            p, q = 1 + i % 3, 1 + i // 3
            for u in range(3):
                away(body, x=p, y=q, z=1 + u, core=1)

        loop(9, step)

    barrier = pltpu.get_barrier_semaphore()

    def first_half(to, device):
        remote(x_ref.at[:, to, 0], got1.at[:, 0, me], send1, recv1.at[0], device).start()

    rounds = (barrier, near_sem.at[0], near_sem.at[1], near_sem.at[2])
    for k, group in enumerate((None, one, two, three)):
        one(
            lambda to, device: pl.semaphore_signal(
                rounds[k], inc=1, device_id=device, device_id_type=MESH
            )
        )
        if group is not None:
            group(first_half)
        pl.semaphore_wait(rounds[k], 10)
    four_apart(first_half)
    everyone(
        lambda to, device: remote(
            x_ref.at[:, to, 1], got1.at[:, 1, me], send1, recv1.at[1], device
        ).start()
    )

    for copy in constants:
        copy.wait()

    n1 = lax.broadcasted_iota(jnp.int32, (128, 128), 0)
    lane = lax.broadcasted_iota(jnp.int32, (128, 128), 1)
    angle = ((8 * me + lane % 8) * (3 * n1 + lane // 8)).astype(F32) * (
        2.0 * math.pi * 128.0 / PADDED
    )
    cosine, sine = jnp.cos(angle), jnp.sin(angle)
    for s in range(3):
        for s8 in range(8):
            at = 8 * s + s8
            column = (
                jnp.broadcast_to(cosine[:, at : at + 1], (128, 128)),
                jnp.broadcast_to(sine[:, at : at + 1], (128, 128)),
            )
            re, im = times(column, (turn[s, 0], turn[s, 1]))
            outer_turn[s, s8, 0] = re
            outer_turn[s, s8, 1] = im
    for a in range(8):
        for part in range(2):
            column_turn[a, part] = jnp.broadcast_to(turn[4, part, :, a : a + 1], (128, 128))
        row = (
            jnp.broadcast_to(turn[5, 0, a : a + 1, :], (128, 128)),
            jnp.broadcast_to(turn[5, 1, a : a + 1, :], (128, 128)),
        )
        re, im = times(row, (turn[3, 0], turn[3, 1]))
        inner_turn[a, 0] = re
        inner_turn[a, 1] = im

    own_in.wait()
    some = pl.ds(0, DEVICES - 1)

    rows1 = got1.reshape(2 * 2 * 128 * 8, 128)
    rows2 = put2.reshape(3 * 2 * 128 * 8, 128)
    from2 = got2.reshape(3 * 2 * 128 * 8, 128)
    rows_out = put3.reshape(3 * 2 * 128 * 8, 128)
    rows3 = got3.reshape(3 * 2 * 128 * 8, 128)
    rows4 = put4.reshape(2 * 2 * 128 * 8, 128)

    def outer_forward(s, t):
        cr = (1.0, -0.5, -0.5)[s]
        ci = (0.0, HALF_ROOT3, -HALF_ROOT3)[s]

        def body(g, carry):
            h = 2 * t + g
            columns = []
            for j in range(2):
                def block(part, upper):
                    at = ((part * 2 + t) * 128 + upper * 64) * 8 + (g * 2 + j) * 2
                    return jnp.concatenate(
                        [rows1[pl.ds(at + e, 64, stride=8), :] for e in range(2)], axis=0
                    )

                x0, x1 = (block(0, 0), block(1, 0)), (block(0, 1), block(1, 1))
                if s == 0:
                    y = add(x0, x1)
                else:
                    y = (
                        x0[0] + cr * x1[0] - ci * x1[1],
                        x0[1] + cr * x1[1] + ci * x1[0],
                    )
                columns.append(jnp.concatenate(y, axis=0))
            out = left(first[s, 0], first[s, 1], jnp.concatenate(columns, axis=1))
            for j in range(2):
                s8 = 2 * h + j
                part = (out[:128, 128 * j : 128 * j + 128], out[128:, 128 * j : 128 * j + 128])
                re, im = times(part, (outer_turn[s, s8, 0], outer_turn[s, s8, 1]))
                at = (s * 2 + t) * 1024 + (g * 2 + j) * 2
                rows2[pl.ds(at, 128, stride=8), :] = re
                rows2[pl.ds(at + 1, 128, stride=8), :] = im
            return carry

        lax.fori_loop(0, 2, body, 0)

    def wait1(t):
        here(x_ref.at[:, some, t], got1.at[:, t, some], send1, recv1.at[t]).wait_recv()

    def give2(s, t):
        got2[s, t, me] = put2[s, t, me]
        everyone(
            lambda to, device: remote(
                put2.at[s, t, to], got2.at[s, t, me], send2, recv2.at[s], device
            ).start()
        )

    def give2_both(s):
        got2[s, :, me] = put2[s, :, me]
        everyone(
            lambda to, device: remote(
                put2.at[s, :, to], got2.at[s, :, me], send2, recv2.at[s], device
            ).start()
        )

    for t in range(2):
        wait1(t)
        outer_forward(0, t)
        give2(0, t)
    for s in (1, 2):
        outer_forward(s, 0)
        outer_forward(s, 1)
        give2_both(s)

    def inner(s):
        def open_eight(i, carry):
            at = pl.multiple_of(16 * i, 16)
            start = (s * 2 + i // 4) * 1024 + i % 4 * 32
            v = [
                tuple(from2[pl.ds(start + 128 * a + part, 16, stride=2), :] for part in range(2))
                for a in range(8)
            ]
            for a, y in enumerate(eight(v, 1)):
                if a:
                    y = times(y, (column_turn[a, 0, pl.ds(at, 16), :], column_turn[a, 1, pl.ds(at, 16), :]))
                for part in range(2):
                    up, down = split(y[part])
                    high[a, pl.ds(128 * part + at, 16), :] = up
                    low[a, pl.ds(128 * part + at, 16), :] = down
            return carry

        lax.fori_loop(0, 8, open_eight, 0)

        def middle(h, carry):
            pair = (2 * h, 2 * h + 1)
            up = jnp.concatenate([high[a] for a in pair], axis=1)
            down = jnp.concatenate([low[a] for a in pair], axis=1)
            out = dot(fg[0, 0], up) + dot(fg[0, 0], down) + dot(fg[0, 1], up)
            lines = []
            for j, a in enumerate(pair):
                y = (out[:128, 128 * j : 128 * j + 128], out[128:, 128 * j : 128 * j + 128])
                re, im = times(y, (inner_turn[a, 0], inner_turn[a, 1]))
                lines.append(jnp.concatenate((re, -im), axis=1))
            v = right(jnp.concatenate(lines, axis=0), fg[0, 0], fg[0, 1])
            re, im = v[:, :128], v[:, 128:]
            squared = jnp.concatenate([(re + im) * (re - im), 2.0 * re * im], axis=1)
            v = right(squared, fg[1, 0], fg[1, 1])
            columns = []
            for j, a in enumerate(pair):
                y = (v[128 * j : 128 * j + 128, :128], v[128 * j : 128 * j + 128, 128:])
                re, im = times(y, (inner_turn[a, 0], inner_turn[a, 1]))
                columns.append(jnp.concatenate((re, -im), axis=0))
            out = left(fg[1, 0], fg[1, 1], jnp.concatenate(columns, axis=1))
            for j, a in enumerate(pair):
                y = (out[:128, 128 * j : 128 * j + 128], out[128:, 128 * j : 128 * j + 128])
                re, im = times_conj(y, (column_turn[a, 0], column_turn[a, 1]))
                back[a, 0] = re
                back[a, 1] = im
            return carry

        lax.fori_loop(0, 4, middle, 0)

        def close_eight(i, carry):
            at = pl.multiple_of(16 * i, 16)
            start = (s * 2 + i // 4) * 1024 + i % 4 * 32
            v = [(back[a, 0, pl.ds(at, 16), :], back[a, 1, pl.ds(at, 16), :]) for a in range(8)]
            for a, y in enumerate(eight(v, -1)):
                for part in range(2):
                    rows_out[pl.ds(start + 128 * a + part, 16, stride=2), :] = y[part]
            return carry

        lax.fori_loop(0, 8, close_eight, 0)

    for s in range(3):
        here(put2.at[s, :, some], got2.at[s, :, some], send2, recv2.at[s]).wait_recv()
        inner(s)
        got3[s, :, me] = put3[s, :, me]
        if s < 2:
            everyone(
                lambda to, device: remote(
                    put3.at[s, :, to], got3.at[s, :, me], send3, recv3.at[s], device
                ).start()
            )
        else:
            for t in range(2):
                everyone(
                    lambda to, device: remote(
                        put3.at[s, t, to], got3.at[s, t, me], send3, recv3.at[s + t], device
                    ).start()
                )

    def outer_backward(s, h):
        columns = []
        for j in range(2):
            s8 = 2 * h + j
            at = (s * 2 + h // 2) * 1024 + (h % 2 * 2 + j) * 2
            z = tuple(rows3[pl.ds(at + part, 128, stride=8), :] for part in range(2))
            z = times_conj(z, (outer_turn[s, s8, 0], outer_turn[s, s8, 1]))
            columns.append(jnp.concatenate(z, axis=0))
        return left(last[s, 0], last[s, 1], jnp.concatenate(columns, axis=1))

    for s in range(2):
        here(put3.at[s, :, some], got3.at[s, :, some], send3, recv3.at[s]).wait_recv()

        def keep(h, carry):
            held[s, h] = outer_backward(s, h)
            return carry

        lax.fori_loop(0, 4, keep, 0)

    own_out = []
    for t in range(2):
        here(put3.at[2, t, some], got3.at[2, t, some], send3, recv3.at[2 + t]).wait_recv()

        def finish(g, carry):
            h = 2 * t + g
            y0, y1, y2 = held[0, h], held[1, h], outer_backward(2, h)
            u, v = y1 + y2, HALF_ROOT3 * (y1 - y2)
            y = y0 - 0.5 * u
            re, im, vr, vi = y[:128], y[128:], v[:128], v[128:]
            for upper, out in enumerate(((re + vi, im - vr), (re - vi, im + vr))):
                for part in range(2):
                    for j in range(2):
                        for e in range(2):
                            at = ((part * 2 + t) * 128 + upper * 64) * 8 + (g * 2 + j) * 2 + e
                            rows4[pl.ds(at, 64, stride=8), :] = out[part][
                                64 * e : 64 * e + 64, 128 * j : 128 * j + 128
                            ]
            return carry

        lax.fori_loop(0, 2, finish, 0)
        own = pltpu.make_async_copy(put4.at[:, t, me], o_ref.at[:, me, t], own_sem.at[1 + t])
        own.start()
        own_out.append(own)
        everyone(
            lambda to, device: remote(
                put4.at[:, t, to], o_ref.at[:, me, t], send4, recv4.at[t], device
            ).start()
        )

    for own in own_out:
        own.wait()
    here(x_ref.at[:, some], got1.at[:, :, some], send1, recv1.at[0]).wait_send()
    for s in range(3):
        here(put2.at[s, :, some], got2.at[s, :, some], send2, recv2.at[s]).wait_send()
        here(put3.at[s, :, some], got3.at[s, :, some], send3, recv3.at[s]).wait_send()
    for t in range(2):
        here(put4.at[:, t, some], o_ref.at[:, some, t], send4, recv4.at[t]).wait()


def hand_over(in_ref, o_ref, sem):
    copy = pltpu.make_async_copy(in_ref, o_ref, sem)
    copy.start()
    copy.wait()


def solution(mesh):
    constants = tables()

    def on_device(modes):
        x = modes.reshape(2, 2, 1024, 128).transpose(0, 2, 1, 3).reshape(2, 128, 2, 8, 128)
        anywhere = pl.BlockSpec(memory_space=pl.ANY)
        dma = pltpu.SemaphoreType.DMA
        out = pl.pallas_call(
            kernel,
            out_shape=pltpu.VMEM((2, 128, 2, 8, 128), F32),
            in_specs=[anywhere] * 5,
            out_specs=pl.BlockSpec(memory_space=pltpu.VMEM),
            scratch_shapes=[
                pltpu.VMEM((3, 2, 256, 256), BF16),
                pltpu.VMEM((3, 2, 256, 256), BF16),
                pltpu.VMEM((2, 2, 256, 256), BF16),
                pltpu.VMEM((6, 2, 128, 128), F32),
                pltpu.VMEM((2, 2, 128, 8, 128), F32),
                pltpu.VMEM((3, 2, 128, 8, 128), F32),
                pltpu.VMEM((3, 2, 128, 8, 128), F32),
                pltpu.VMEM((3, 2, 128, 8, 128), F32),
                pltpu.VMEM((3, 2, 128, 8, 128), F32),
                pltpu.VMEM((2, 2, 128, 8, 128), F32),
                pltpu.VMEM((3, 8, 2, 128, 128), F32),
                pltpu.VMEM((8, 2, 128, 128), F32),
                pltpu.VMEM((8, 2, 128, 128), F32),
                pltpu.VMEM((8, 256, 128), BF16),
                pltpu.VMEM((8, 256, 128), BF16),
                pltpu.VMEM((8, 2, 128, 128), F32),
                pltpu.VMEM((2, 4, 256, 256), F32),
                pltpu.SemaphoreType.REGULAR((3,)),
                dma((4,)),
                dma((3,)),
                dma,
                dma((2,)),
                dma,
                dma((3,)),
                dma,
                dma((4,)),
                dma,
                dma((2,)),
            ],
            compiler_params=pltpu.CompilerParams(
                collective_id=0, has_side_effects=True, vmem_limit_bytes=67043328 - 2**21 - 2**17
            ),
        )(x, *(jnp.asarray(c) for c in constants))
        out = pl.pallas_call(
            hand_over,
            out_shape=jax.ShapeDtypeStruct((2, 128, 2, 8, 128), F32),
            in_specs=[pl.BlockSpec(memory_space=pltpu.VMEM)],
            out_specs=anywhere,
            scratch_shapes=[dma],
            compiler_params=pltpu.CompilerParams(vmem_limit_bytes=2**17),
        )(out)
        return out.reshape(2, 1024, 2, 128).transpose(0, 2, 1, 3).reshape(2, 2, LOCAL)

    spec = P(None, "res", "blk")
    return jax.shard_map(on_device, mesh=mesh, in_specs=(spec,), out_specs=spec, check_vma=False)
```

```python
import math

import jax
import jax.numpy as jnp
import numpy as np
from jax import lax
from jax.experimental import pallas as pl
from jax.experimental.pallas import tpu as pltpu
from jax.sharding import PartitionSpec as P

F32, BF16 = jnp.float32, jnp.bfloat16
DEVICES = 128
PADDED = 50331648
LOCAL = 131072
STEP = 37
MESH = pl.DeviceIdType.MESH
HALF_ROOT3 = math.sqrt(3.0) / 2.0
ROOT_HALF = math.sqrt(0.5)


def real_block(w):
    return np.block([[w.real, -w.imag], [w.imag, w.real]])


def high_low(w):
    high = np.asarray(w, np.float32).astype(jnp.bfloat16)
    low = (w - high.astype(np.float64)).astype(np.float32).astype(jnp.bfloat16)
    return np.stack([high, low])


def root(turns):
    return np.exp(2j * np.pi * (turns % 1.0))


def tables():
    n = np.arange(128)
    kl = np.array([(u // 32) * 64 + e * 32 + u % 32 for e in range(2) for u in range(64)])
    first, last = [], []
    for s in range(3):
        w = root(np.outer(n, kl) / 128.0) * root(kl * s / 384.0)[None, :]
        first.append(high_low(real_block(w)))
        last.append(high_low(real_block(w).T / PADDED))
    mixed = (n % 64) // 4 * 8 + n // 64 * 4 + n % 4
    f = real_block(root(np.outer(n, mixed) / 128.0))
    turn = [root(np.outer(3 * n + s, n) / PADDED) for s in range(3)]
    turn.append(root(np.outer(n, n) / 16384.0))
    columns = np.zeros((128, 128), np.complex128)
    columns[:, :8] = root(np.outer(mixed, np.arange(8)) / 1024.0)
    turn.append(columns)
    rows = np.zeros((128, 128), np.complex128)
    rows[:8] = root(np.outer(np.arange(8), n) / LOCAL)
    turn.append(rows)
    turn = np.stack([np.stack([t.real, t.imag]) for t in turn]).astype(np.float32)
    return (
        np.stack(first),
        np.stack(last),
        np.stack([high_low(f), high_low(f.T)]),
        turn,
    )


def split(x):
    high = x.astype(BF16)
    return high, (x - high.astype(F32)).astype(BF16)


def dot(a, b):
    return jnp.dot(a, b, preferred_element_type=F32)


def left(w_high, w_low, x):
    high, low = split(x)
    return dot(w_high, high) + dot(w_high, low) + dot(w_low, high)


def right(x, w_high, w_low):
    high, low = split(x)
    return dot(high, w_high) + dot(low, w_high) + dot(high, w_low)


def times(a, b):
    return a[0] * b[0] - a[1] * b[1], a[0] * b[1] + a[1] * b[0]


def times_conj(a, b):
    return a[0] * b[0] + a[1] * b[1], a[1] * b[0] - a[0] * b[1]


def add(a, b):
    return a[0] + b[0], a[1] + b[1]


def sub(a, b):
    return a[0] - b[0], a[1] - b[1]


def quarter(a, sign):
    return (-a[1], a[0]) if sign > 0 else (a[1], -a[0])


def eighth(a, sign):
    if sign > 0:
        return (a[0] - a[1]) * ROOT_HALF, (a[0] + a[1]) * ROOT_HALF
    return (a[0] + a[1]) * ROOT_HALF, (a[1] - a[0]) * ROOT_HALF


def four(a, b, c, d, sign):
    p, q, r, t = add(a, c), sub(a, c), add(b, d), quarter(sub(b, d), sign)
    return add(p, r), add(q, t), sub(p, r), sub(q, t)


def eight(v, sign):
    even = four(v[0], v[2], v[4], v[6], sign)
    odd = four(v[1], v[3], v[5], v[7], sign)
    odd = (
        odd[0],
        eighth(odd[1], sign),
        quarter(odd[2], sign),
        quarter(eighth(odd[3], sign), sign),
    )
    return [add(e, o) for e, o in zip(even, odd)] + [sub(e, o) for e, o in zip(even, odd)]


def kernel(
    x_ref, first_hbm, last_hbm, fg_hbm, turn_hbm, o_ref,
    first, last, fg, turn, got1, put2, got2, put3, got3, put4,
    outer_turn, column_turn, inner_turn, high, low, back, held,
    near_sem, const_sem, own_sem, send1, recv1, send2, recv2, send3, recv3, send4, recv4,
):
    r, b = lax.axis_index("res"), lax.axis_index("blk")
    me = r * 32 + b

    constants = [
        pltpu.make_async_copy(src, dst, const_sem.at[i])
        for i, (src, dst) in enumerate(
            ((first_hbm, first), (last_hbm, last), (fg_hbm, fg), (turn_hbm, turn))
        )
    ]
    for copy in constants:
        copy.start()
    own_in = pltpu.make_async_copy(x_ref.at[:, me], got1.at[:, :, me], own_sem.at[0])
    own_in.start()

    def remote(src, dst, send, recv, device):
        return pltpu.make_async_remote_copy(
            src_ref=src,
            dst_ref=dst,
            send_sem=send,
            recv_sem=recv,
            device_id=device,
            device_id_type=MESH,
        )

    def here(src, dst, send, recv):
        return remote(src, dst, send, recv, {"res": r, "blk": b})

    def everyone(body):
        def step(i, carry):
            to = (me + i * STEP) % DEVICES
            body(to, {"res": to // 32, "blk": to % 32})
            return carry

        lax.fori_loop(1, DEVICES, step, 0)

    at_x, at_y, at_z, at_core = r // 2 * 2 + b // 16, b // 4 % 4, b % 4, r % 2

    def away(body, x=0, y=0, z=0, core=0):
        to_x = (at_x + x) % 4
        res = to_x // 2 * 2 + (at_core + core) % 2
        blk = to_x % 2 * 16 + (at_y + y) % 4 * 4 + (at_z + z) % 4
        body(res * 32 + blk, {"res": res, "blk": blk})

    def loop(count, body):
        def step(i, carry):
            body(i)
            return carry

        lax.fori_loop(0, count, step, 0)

    def one(body):
        def step(i):
            away(body, x=1 + i)
            away(body, y=1 + i)
            away(body, z=1 + i)

        loop(3, step)
        away(body, core=1)

    def two(body):
        def step(i):
            p, q = 1 + i % 3, 1 + i // 3
            away(body, x=p, y=q)
            away(body, y=p, z=q)
            away(body, z=p, x=q)

        loop(9, step)

        def over(i):
            away(body, x=1 + i, core=1)
            away(body, y=1 + i, core=1)
            away(body, z=1 + i, core=1)

        loop(3, over)

    def three(body):
        def step(i):
            p, q = 1 + i % 3, 1 + i // 3
            for u in range(3):
                away(body, x=p, y=q, z=1 + u)
            away(body, x=p, y=q, core=1)
            away(body, y=p, z=q, core=1)
            away(body, z=p, x=q, core=1)

        loop(9, step)

    def four_apart(body):
        def step(i):
            p, q = 1 + i % 3, 1 + i // 3
            for u in range(3):
                away(body, x=p, y=q, z=1 + u, core=1)

        loop(9, step)

    barrier = pltpu.get_barrier_semaphore()

    def first_half(to, device):
        remote(x_ref.at[:, to, 0], got1.at[:, 0, me], send1, recv1.at[0], device).start()

    rounds = (barrier, near_sem.at[0], near_sem.at[1], near_sem.at[2])
    for k, group in enumerate((None, one, two, three)):
        one(
            lambda to, device: pl.semaphore_signal(
                rounds[k], inc=1, device_id=device, device_id_type=MESH
            )
        )
        if group is not None:
            group(first_half)
        pl.semaphore_wait(rounds[k], 10)
    four_apart(first_half)
    everyone(
        lambda to, device: remote(
            x_ref.at[:, to, 1], got1.at[:, 1, me], send1, recv1.at[1], device
        ).start()
    )

    for copy in constants:
        copy.wait()

    n1 = lax.broadcasted_iota(jnp.int32, (128, 128), 0)
    lane = lax.broadcasted_iota(jnp.int32, (128, 128), 1)
    angle = ((8 * me + lane % 8) * (3 * n1 + lane // 8)).astype(F32) * (
        2.0 * math.pi * 128.0 / PADDED
    )
    cosine, sine = jnp.cos(angle), jnp.sin(angle)
    for s in range(3):
        for s8 in range(8):
            at = 8 * s + s8
            column = (
                jnp.broadcast_to(cosine[:, at : at + 1], (128, 128)),
                jnp.broadcast_to(sine[:, at : at + 1], (128, 128)),
            )
            re, im = times(column, (turn[s, 0], turn[s, 1]))
            outer_turn[s, s8, 0] = re
            outer_turn[s, s8, 1] = im
    for a in range(8):
        for part in range(2):
            column_turn[a, part] = jnp.broadcast_to(turn[4, part, :, a : a + 1], (128, 128))
        row = (
            jnp.broadcast_to(turn[5, 0, a : a + 1, :], (128, 128)),
            jnp.broadcast_to(turn[5, 1, a : a + 1, :], (128, 128)),
        )
        re, im = times(row, (turn[3, 0], turn[3, 1]))
        inner_turn[a, 0] = re
        inner_turn[a, 1] = im

    own_in.wait()
    some = pl.ds(0, DEVICES - 1)

    rows1 = got1.reshape(2 * 2 * 128 * 8, 128)
    rows2 = put2.reshape(3 * 2 * 128 * 8, 128)
    from2 = got2.reshape(3 * 2 * 128 * 8, 128)
    rows_out = put3.reshape(3 * 2 * 128 * 8, 128)
    rows3 = got3.reshape(3 * 2 * 128 * 8, 128)
    rows4 = put4.reshape(2 * 2 * 128 * 8, 128)

    def outer_forward(s, t):
        cr = (1.0, -0.5, -0.5)[s]
        ci = (0.0, HALF_ROOT3, -HALF_ROOT3)[s]

        def body(g, carry):
            h = 2 * t + g
            columns = []
            for j in range(2):
                def block(part, upper):
                    at = ((part * 2 + t) * 128 + upper * 64) * 8 + (g * 2 + j) * 2
                    return jnp.concatenate(
                        [rows1[pl.ds(at + e, 64, stride=8), :] for e in range(2)], axis=0
                    )

                x0, x1 = (block(0, 0), block(1, 0)), (block(0, 1), block(1, 1))
                if s == 0:
                    y = add(x0, x1)
                else:
                    y = (
                        x0[0] + cr * x1[0] - ci * x1[1],
                        x0[1] + cr * x1[1] + ci * x1[0],
                    )
                columns.append(jnp.concatenate(y, axis=0))
            out = left(first[s, 0], first[s, 1], jnp.concatenate(columns, axis=1))
            for j in range(2):
                s8 = 2 * h + j
                part = (out[:128, 128 * j : 128 * j + 128], out[128:, 128 * j : 128 * j + 128])
                re, im = times(part, (outer_turn[s, s8, 0], outer_turn[s, s8, 1]))
                at = (s * 2 + t) * 1024 + (g * 2 + j) * 2
                rows2[pl.ds(at, 128, stride=8), :] = re
                rows2[pl.ds(at + 1, 128, stride=8), :] = im
            return carry

        lax.fori_loop(0, 2, body, 0)

    def wait1(t):
        here(x_ref.at[:, some, t], got1.at[:, t, some], send1, recv1.at[t]).wait_recv()

    def give2(s, t):
        got2[s, t, me] = put2[s, t, me]
        everyone(
            lambda to, device: remote(
                put2.at[s, t, to], got2.at[s, t, me], send2, recv2.at[s], device
            ).start()
        )

    def give2_both(s):
        got2[s, :, me] = put2[s, :, me]
        everyone(
            lambda to, device: remote(
                put2.at[s, :, to], got2.at[s, :, me], send2, recv2.at[s], device
            ).start()
        )

    wait1(0)
    for s in range(2):
        outer_forward(s, 0)
        give2(s, 0)
    wait1(1)
    outer_forward(0, 1)
    give2(0, 1)
    outer_forward(1, 1)
    give2(1, 1)
    for t in range(2):
        outer_forward(2, t)
        give2(2, t)

    def inner(s):
        def open_eight(i, carry):
            at = pl.multiple_of(16 * i, 16)
            start = (s * 2 + i // 4) * 1024 + i % 4 * 32
            v = [
                tuple(from2[pl.ds(start + 128 * a + part, 16, stride=2), :] for part in range(2))
                for a in range(8)
            ]
            for a, y in enumerate(eight(v, 1)):
                if a:
                    y = times(y, (column_turn[a, 0, pl.ds(at, 16), :], column_turn[a, 1, pl.ds(at, 16), :]))
                for part in range(2):
                    up, down = split(y[part])
                    high[a, pl.ds(128 * part + at, 16), :] = up
                    low[a, pl.ds(128 * part + at, 16), :] = down
            return carry

        lax.fori_loop(0, 8, open_eight, 0)

        def middle(h, carry):
            pair = (2 * h, 2 * h + 1)
            up = jnp.concatenate([high[a] for a in pair], axis=1)
            down = jnp.concatenate([low[a] for a in pair], axis=1)
            out = dot(fg[0, 0], up) + dot(fg[0, 0], down) + dot(fg[0, 1], up)
            lines = []
            for j, a in enumerate(pair):
                y = (out[:128, 128 * j : 128 * j + 128], out[128:, 128 * j : 128 * j + 128])
                re, im = times(y, (inner_turn[a, 0], inner_turn[a, 1]))
                lines.append(jnp.concatenate((re, -im), axis=1))
            v = right(jnp.concatenate(lines, axis=0), fg[0, 0], fg[0, 1])
            re, im = v[:, :128], v[:, 128:]
            squared = jnp.concatenate([(re + im) * (re - im), 2.0 * re * im], axis=1)
            v = right(squared, fg[1, 0], fg[1, 1])
            columns = []
            for j, a in enumerate(pair):
                y = (v[128 * j : 128 * j + 128, :128], v[128 * j : 128 * j + 128, 128:])
                re, im = times(y, (inner_turn[a, 0], inner_turn[a, 1]))
                columns.append(jnp.concatenate((re, -im), axis=0))
            out = left(fg[1, 0], fg[1, 1], jnp.concatenate(columns, axis=1))
            for j, a in enumerate(pair):
                y = (out[:128, 128 * j : 128 * j + 128], out[128:, 128 * j : 128 * j + 128])
                re, im = times_conj(y, (column_turn[a, 0], column_turn[a, 1]))
                back[a, 0] = re
                back[a, 1] = im
            return carry

        lax.fori_loop(0, 4, middle, 0)

        def close_eight(i, carry):
            at = pl.multiple_of(16 * i, 16)
            start = (s * 2 + i // 4) * 1024 + i % 4 * 32
            v = [(back[a, 0, pl.ds(at, 16), :], back[a, 1, pl.ds(at, 16), :]) for a in range(8)]
            for a, y in enumerate(eight(v, -1)):
                for part in range(2):
                    rows_out[pl.ds(start + 128 * a + part, 16, stride=2), :] = y[part]
            return carry

        lax.fori_loop(0, 8, close_eight, 0)

    for s in range(3):
        here(put2.at[s, :, some], got2.at[s, :, some], send2, recv2.at[s]).wait_recv()
        inner(s)
        got3[s, :, me] = put3[s, :, me]
        if s < 2:
            everyone(
                lambda to, device: remote(
                    put3.at[s, :, to], got3.at[s, :, me], send3, recv3.at[s], device
                ).start()
            )
        else:
            for t in range(2):
                everyone(
                    lambda to, device: remote(
                        put3.at[s, t, to], got3.at[s, t, me], send3, recv3.at[s + t], device
                    ).start()
                )

    def outer_backward(s, h):
        columns = []
        for j in range(2):
            s8 = 2 * h + j
            at = (s * 2 + h // 2) * 1024 + (h % 2 * 2 + j) * 2
            z = tuple(rows3[pl.ds(at + part, 128, stride=8), :] for part in range(2))
            z = times_conj(z, (outer_turn[s, s8, 0], outer_turn[s, s8, 1]))
            columns.append(jnp.concatenate(z, axis=0))
        return left(last[s, 0], last[s, 1], jnp.concatenate(columns, axis=1))

    for s in range(2):
        here(put3.at[s, :, some], got3.at[s, :, some], send3, recv3.at[s]).wait_recv()

        def keep(h, carry):
            held[s, h] = outer_backward(s, h)
            return carry

        lax.fori_loop(0, 4, keep, 0)

    own_out = []
    for t in range(2):
        here(put3.at[2, t, some], got3.at[2, t, some], send3, recv3.at[2 + t]).wait_recv()

        def finish(g, carry):
            h = 2 * t + g
            y0, y1, y2 = held[0, h], held[1, h], outer_backward(2, h)
            u, v = y1 + y2, HALF_ROOT3 * (y1 - y2)
            y = y0 - 0.5 * u
            re, im, vr, vi = y[:128], y[128:], v[:128], v[128:]
            for upper, out in enumerate(((re + vi, im - vr), (re - vi, im + vr))):
                for part in range(2):
                    for j in range(2):
                        for e in range(2):
                            at = ((part * 2 + t) * 128 + upper * 64) * 8 + (g * 2 + j) * 2 + e
                            rows4[pl.ds(at, 64, stride=8), :] = out[part][
                                64 * e : 64 * e + 64, 128 * j : 128 * j + 128
                            ]
            return carry

        lax.fori_loop(0, 2, finish, 0)
        own = pltpu.make_async_copy(put4.at[:, t, me], o_ref.at[:, me, t], own_sem.at[1 + t])
        own.start()
        own_out.append(own)
        everyone(
            lambda to, device: remote(
                put4.at[:, t, to], o_ref.at[:, me, t], send4, recv4.at[t], device
            ).start()
        )

    for own in own_out:
        own.wait()
    here(x_ref.at[:, some], got1.at[:, :, some], send1, recv1.at[0]).wait_send()
    for s in range(3):
        here(put2.at[s, :, some], got2.at[s, :, some], send2, recv2.at[s]).wait_send()
        here(put3.at[s, :, some], got3.at[s, :, some], send3, recv3.at[s]).wait_send()
    for t in range(2):
        here(put4.at[:, t, some], o_ref.at[:, some, t], send4, recv4.at[t]).wait()


def hand_over(in_ref, o_ref, sem):
    copy = pltpu.make_async_copy(in_ref, o_ref, sem)
    copy.start()
    copy.wait()


def solution(mesh):
    constants = tables()

    def on_device(modes):
        x = modes.reshape(2, 2, 1024, 128).transpose(0, 2, 1, 3).reshape(2, 128, 2, 8, 128)
        anywhere = pl.BlockSpec(memory_space=pl.ANY)
        dma = pltpu.SemaphoreType.DMA
        out = pl.pallas_call(
            kernel,
            out_shape=pltpu.VMEM((2, 128, 2, 8, 128), F32),
            in_specs=[anywhere] * 5,
            out_specs=pl.BlockSpec(memory_space=pltpu.VMEM),
            scratch_shapes=[
                pltpu.VMEM((3, 2, 256, 256), BF16),
                pltpu.VMEM((3, 2, 256, 256), BF16),
                pltpu.VMEM((2, 2, 256, 256), BF16),
                pltpu.VMEM((6, 2, 128, 128), F32),
                pltpu.VMEM((2, 2, 128, 8, 128), F32),
                pltpu.VMEM((3, 2, 128, 8, 128), F32),
                pltpu.VMEM((3, 2, 128, 8, 128), F32),
                pltpu.VMEM((3, 2, 128, 8, 128), F32),
                pltpu.VMEM((3, 2, 128, 8, 128), F32),
                pltpu.VMEM((2, 2, 128, 8, 128), F32),
                pltpu.VMEM((3, 8, 2, 128, 128), F32),
                pltpu.VMEM((8, 2, 128, 128), F32),
                pltpu.VMEM((8, 2, 128, 128), F32),
                pltpu.VMEM((8, 256, 128), BF16),
                pltpu.VMEM((8, 256, 128), BF16),
                pltpu.VMEM((8, 2, 128, 128), F32),
                pltpu.VMEM((2, 4, 256, 256), F32),
                pltpu.SemaphoreType.REGULAR((3,)),
                dma((4,)),
                dma((3,)),
                dma,
                dma((2,)),
                dma,
                dma((3,)),
                dma,
                dma((4,)),
                dma,
                dma((2,)),
            ],
            compiler_params=pltpu.CompilerParams(
                collective_id=0, has_side_effects=True, vmem_limit_bytes=67043328 - 2**21 - 2**17
            ),
        )(x, *(jnp.asarray(c) for c in constants))
        out = pl.pallas_call(
            hand_over,
            out_shape=jax.ShapeDtypeStruct((2, 128, 2, 8, 128), F32),
            in_specs=[pl.BlockSpec(memory_space=pltpu.VMEM)],
            out_specs=anywhere,
            scratch_shapes=[dma],
            compiler_params=pltpu.CompilerParams(vmem_limit_bytes=2**17),
        )(out)
        return out.reshape(2, 1024, 2, 128).transpose(0, 2, 1, 3).reshape(2, 2, LOCAL)

    spec = P(None, "res", "blk")
    return jax.shard_map(on_device, mesh=mesh, in_specs=(spec,), out_specs=spec, check_vma=False)
```

```python
import math

import jax
import jax.numpy as jnp
import numpy as np
from jax import lax
from jax.experimental import pallas as pl
from jax.experimental.pallas import tpu as pltpu
from jax.sharding import PartitionSpec as P

F32, BF16 = jnp.float32, jnp.bfloat16
DEVICES = 128
PADDED = 50331648
LOCAL = 131072
STEP = 37
MESH = pl.DeviceIdType.MESH
HALF_ROOT3 = math.sqrt(3.0) / 2.0
ROOT_HALF = math.sqrt(0.5)


def real_block(w):
    return np.block([[w.real, -w.imag], [w.imag, w.real]])


def high_low(w):
    high = np.asarray(w, np.float32).astype(jnp.bfloat16)
    low = (w - high.astype(np.float64)).astype(np.float32).astype(jnp.bfloat16)
    return np.stack([high, low])


def root(turns):
    return np.exp(2j * np.pi * (turns % 1.0))


def tables():
    n = np.arange(128)
    kl = np.array([(u // 32) * 64 + e * 32 + u % 32 for e in range(2) for u in range(64)])
    first, last = [], []
    for s in range(3):
        w = root(np.outer(n, kl) / 128.0) * root(kl * s / 384.0)[None, :]
        first.append(high_low(real_block(w)))
        last.append(high_low(real_block(w).T / PADDED))
    mixed = (n % 64) // 4 * 8 + n // 64 * 4 + n % 4
    f = real_block(root(np.outer(n, mixed) / 128.0))
    turn = [root(np.outer(3 * n + s, n) / PADDED) for s in range(3)]
    turn.append(root(np.outer(n, n) / 16384.0))
    columns = np.zeros((128, 128), np.complex128)
    columns[:, :8] = root(np.outer(mixed, np.arange(8)) / 1024.0)
    turn.append(columns)
    rows = np.zeros((128, 128), np.complex128)
    rows[:8] = root(np.outer(np.arange(8), n) / LOCAL)
    turn.append(rows)
    turn = np.stack([np.stack([t.real, t.imag]) for t in turn]).astype(np.float32)
    return (
        np.stack(first),
        np.stack(last),
        np.stack([high_low(f), high_low(f.T)]),
        turn,
    )


def split(x):
    high = x.astype(BF16)
    return high, (x - high.astype(F32)).astype(BF16)


def dot(a, b):
    return jnp.dot(a, b, preferred_element_type=F32)


def left(w_high, w_low, x):
    high, low = split(x)
    return dot(w_high, high) + dot(w_high, low) + dot(w_low, high)


def right(x, w_high, w_low):
    high, low = split(x)
    return dot(high, w_high) + dot(low, w_high) + dot(high, w_low)


def times(a, b):
    return a[0] * b[0] - a[1] * b[1], a[0] * b[1] + a[1] * b[0]


def times_conj(a, b):
    return a[0] * b[0] + a[1] * b[1], a[1] * b[0] - a[0] * b[1]


def add(a, b):
    return a[0] + b[0], a[1] + b[1]


def sub(a, b):
    return a[0] - b[0], a[1] - b[1]


def quarter(a, sign):
    return (-a[1], a[0]) if sign > 0 else (a[1], -a[0])


def eighth(a, sign):
    if sign > 0:
        return (a[0] - a[1]) * ROOT_HALF, (a[0] + a[1]) * ROOT_HALF
    return (a[0] + a[1]) * ROOT_HALF, (a[1] - a[0]) * ROOT_HALF


def four(a, b, c, d, sign):
    p, q, r, t = add(a, c), sub(a, c), add(b, d), quarter(sub(b, d), sign)
    return add(p, r), add(q, t), sub(p, r), sub(q, t)


def eight(v, sign):
    even = four(v[0], v[2], v[4], v[6], sign)
    odd = four(v[1], v[3], v[5], v[7], sign)
    odd = (
        odd[0],
        eighth(odd[1], sign),
        quarter(odd[2], sign),
        quarter(eighth(odd[3], sign), sign),
    )
    return [add(e, o) for e, o in zip(even, odd)] + [sub(e, o) for e, o in zip(even, odd)]


def kernel(
    x_ref, first_hbm, last_hbm, fg_hbm, turn_hbm, o_ref,
    first, last, fg, turn, got1, put2, got2, put3, got3, put4,
    outer_turn, column_turn, inner_turn, high, low, back, held,
    near_sem, const_sem, own_sem, send1, recv1, send2, recv2, send3, recv3, send4, recv4,
):
    r, b = lax.axis_index("res"), lax.axis_index("blk")
    me = r * 32 + b

    constants = [
        pltpu.make_async_copy(src, dst, const_sem.at[i])
        for i, (src, dst) in enumerate(
            ((first_hbm, first), (last_hbm, last), (fg_hbm, fg), (turn_hbm, turn))
        )
    ]
    own_in = pltpu.make_async_copy(x_ref.at[:, me], got1.at[:, :, me], own_sem.at[0])

    def remote(src, dst, send, recv, device):
        return pltpu.make_async_remote_copy(
            src_ref=src,
            dst_ref=dst,
            send_sem=send,
            recv_sem=recv,
            device_id=device,
            device_id_type=MESH,
        )

    def here(src, dst, send, recv):
        return remote(src, dst, send, recv, {"res": r, "blk": b})

    def everyone(body):
        def step(i, carry):
            to = (me + i * STEP) % DEVICES
            body(to, {"res": to // 32, "blk": to % 32})
            return carry

        lax.fori_loop(1, DEVICES, step, 0)

    at_x, at_y, at_z, at_core = r // 2 * 2 + b // 16, b // 4 % 4, b % 4, r % 2

    def away(body, x=0, y=0, z=0, core=0):
        to_x = (at_x + x) % 4
        res = to_x // 2 * 2 + (at_core + core) % 2
        blk = to_x % 2 * 16 + (at_y + y) % 4 * 4 + (at_z + z) % 4
        body(res * 32 + blk, {"res": res, "blk": blk})

    def loop(count, body):
        def step(i, carry):
            body(i)
            return carry

        lax.fori_loop(0, count, step, 0)

    def one(body):
        def step(i):
            away(body, x=1 + i)
            away(body, y=1 + i)
            away(body, z=1 + i)

        loop(3, step)
        away(body, core=1)

    def two(body):
        def step(i):
            p, q = 1 + i % 3, 1 + i // 3
            away(body, x=p, y=q)
            away(body, y=p, z=q)
            away(body, z=p, x=q)

        loop(9, step)

        def over(i):
            away(body, x=1 + i, core=1)
            away(body, y=1 + i, core=1)
            away(body, z=1 + i, core=1)

        loop(3, over)

    def three(body):
        def step(i):
            p, q = 1 + i % 3, 1 + i // 3
            for u in range(3):
                away(body, x=p, y=q, z=1 + u)
            away(body, x=p, y=q, core=1)
            away(body, y=p, z=q, core=1)
            away(body, z=p, x=q, core=1)

        loop(9, step)

    def four_apart(body):
        def step(i):
            p, q = 1 + i % 3, 1 + i // 3
            for u in range(3):
                away(body, x=p, y=q, z=1 + u, core=1)

        loop(9, step)

    barrier = pltpu.get_barrier_semaphore()

    def first_half(to, device):
        remote(x_ref.at[:, to, 0], got1.at[:, 0, me], send1, recv1.at[0], device).start()

    rounds = (barrier, near_sem.at[0], near_sem.at[1], near_sem.at[2])
    for k, group in enumerate((None, one, two, three)):
        one(
            lambda to, device: pl.semaphore_signal(
                rounds[k], inc=1, device_id=device, device_id_type=MESH
            )
        )
        if group is not None:
            group(first_half)
        else:
            for copy in constants:
                copy.start()
            own_in.start()
        pl.semaphore_wait(rounds[k], 10)
    four_apart(first_half)
    everyone(
        lambda to, device: remote(
            x_ref.at[:, to, 1], got1.at[:, 1, me], send1, recv1.at[1], device
        ).start()
    )

    for copy in constants:
        copy.wait()

    n1 = lax.broadcasted_iota(jnp.int32, (128, 128), 0)
    lane = lax.broadcasted_iota(jnp.int32, (128, 128), 1)
    angle = ((8 * me + lane % 8) * (3 * n1 + lane // 8)).astype(F32) * (
        2.0 * math.pi * 128.0 / PADDED
    )
    cosine, sine = jnp.cos(angle), jnp.sin(angle)
    for s in range(3):
        for s8 in range(8):
            at = 8 * s + s8
            column = (
                jnp.broadcast_to(cosine[:, at : at + 1], (128, 128)),
                jnp.broadcast_to(sine[:, at : at + 1], (128, 128)),
            )
            re, im = times(column, (turn[s, 0], turn[s, 1]))
            outer_turn[s, s8, 0] = re
            outer_turn[s, s8, 1] = im
    for a in range(8):
        for part in range(2):
            column_turn[a, part] = jnp.broadcast_to(turn[4, part, :, a : a + 1], (128, 128))
        row = (
            jnp.broadcast_to(turn[5, 0, a : a + 1, :], (128, 128)),
            jnp.broadcast_to(turn[5, 1, a : a + 1, :], (128, 128)),
        )
        re, im = times(row, (turn[3, 0], turn[3, 1]))
        inner_turn[a, 0] = re
        inner_turn[a, 1] = im

    own_in.wait()
    some = pl.ds(0, DEVICES - 1)

    rows1 = got1.reshape(2 * 2 * 128 * 8, 128)
    rows2 = put2.reshape(3 * 2 * 128 * 8, 128)
    from2 = got2.reshape(3 * 2 * 128 * 8, 128)
    rows_out = put3.reshape(3 * 2 * 128 * 8, 128)
    rows3 = got3.reshape(3 * 2 * 128 * 8, 128)
    rows4 = put4.reshape(2 * 2 * 128 * 8, 128)

    def outer_forward(s, t):
        cr = (1.0, -0.5, -0.5)[s]
        ci = (0.0, HALF_ROOT3, -HALF_ROOT3)[s]

        def body(g, carry):
            h = 2 * t + g
            columns = []
            for j in range(2):
                def block(part, upper):
                    at = ((part * 2 + t) * 128 + upper * 64) * 8 + (g * 2 + j) * 2
                    return jnp.concatenate(
                        [rows1[pl.ds(at + e, 64, stride=8), :] for e in range(2)], axis=0
                    )

                x0, x1 = (block(0, 0), block(1, 0)), (block(0, 1), block(1, 1))
                if s == 0:
                    y = add(x0, x1)
                else:
                    y = (
                        x0[0] + cr * x1[0] - ci * x1[1],
                        x0[1] + cr * x1[1] + ci * x1[0],
                    )
                columns.append(jnp.concatenate(y, axis=0))
            out = left(first[s, 0], first[s, 1], jnp.concatenate(columns, axis=1))
            for j in range(2):
                s8 = 2 * h + j
                part = (out[:128, 128 * j : 128 * j + 128], out[128:, 128 * j : 128 * j + 128])
                re, im = times(part, (outer_turn[s, s8, 0], outer_turn[s, s8, 1]))
                at = (s * 2 + t) * 1024 + (g * 2 + j) * 2
                rows2[pl.ds(at, 128, stride=8), :] = re
                rows2[pl.ds(at + 1, 128, stride=8), :] = im
            return carry

        lax.fori_loop(0, 2, body, 0)

    def wait1(t):
        here(x_ref.at[:, some, t], got1.at[:, t, some], send1, recv1.at[t]).wait_recv()

    def give2(s, t):
        got2[s, t, me] = put2[s, t, me]
        everyone(
            lambda to, device: remote(
                put2.at[s, t, to], got2.at[s, t, me], send2, recv2.at[s], device
            ).start()
        )

    def give2_both(s):
        got2[s, :, me] = put2[s, :, me]
        everyone(
            lambda to, device: remote(
                put2.at[s, :, to], got2.at[s, :, me], send2, recv2.at[s], device
            ).start()
        )

    wait1(0)
    for s in range(2):
        outer_forward(s, 0)
        give2(s, 0)
    wait1(1)
    outer_forward(0, 1)
    give2(0, 1)
    outer_forward(1, 1)
    give2(1, 1)
    for t in range(2):
        outer_forward(2, t)
        give2(2, t)

    def inner(s):
        def open_eight(i, carry):
            at = pl.multiple_of(16 * i, 16)
            start = (s * 2 + i // 4) * 1024 + i % 4 * 32
            v = [
                tuple(from2[pl.ds(start + 128 * a + part, 16, stride=2), :] for part in range(2))
                for a in range(8)
            ]
            for a, y in enumerate(eight(v, 1)):
                if a:
                    y = times(y, (column_turn[a, 0, pl.ds(at, 16), :], column_turn[a, 1, pl.ds(at, 16), :]))
                for part in range(2):
                    up, down = split(y[part])
                    high[a, pl.ds(128 * part + at, 16), :] = up
                    low[a, pl.ds(128 * part + at, 16), :] = down
            return carry

        lax.fori_loop(0, 8, open_eight, 0)

        def middle(h, carry):
            pair = (2 * h, 2 * h + 1)
            up = jnp.concatenate([high[a] for a in pair], axis=1)
            down = jnp.concatenate([low[a] for a in pair], axis=1)
            out = dot(fg[0, 0], up) + dot(fg[0, 0], down) + dot(fg[0, 1], up)
            lines = []
            for j, a in enumerate(pair):
                y = (out[:128, 128 * j : 128 * j + 128], out[128:, 128 * j : 128 * j + 128])
                re, im = times(y, (inner_turn[a, 0], inner_turn[a, 1]))
                lines.append(jnp.concatenate((re, -im), axis=1))
            v = right(jnp.concatenate(lines, axis=0), fg[0, 0], fg[0, 1])
            re, im = v[:, :128], v[:, 128:]
            squared = jnp.concatenate([(re + im) * (re - im), 2.0 * re * im], axis=1)
            v = right(squared, fg[1, 0], fg[1, 1])
            columns = []
            for j, a in enumerate(pair):
                y = (v[128 * j : 128 * j + 128, :128], v[128 * j : 128 * j + 128, 128:])
                re, im = times(y, (inner_turn[a, 0], inner_turn[a, 1]))
                columns.append(jnp.concatenate((re, -im), axis=0))
            out = left(fg[1, 0], fg[1, 1], jnp.concatenate(columns, axis=1))
            for j, a in enumerate(pair):
                y = (out[:128, 128 * j : 128 * j + 128], out[128:, 128 * j : 128 * j + 128])
                re, im = times_conj(y, (column_turn[a, 0], column_turn[a, 1]))
                back[a, 0] = re
                back[a, 1] = im
            return carry

        lax.fori_loop(0, 4, middle, 0)

        def close_eight(i, carry):
            at = pl.multiple_of(16 * i, 16)
            start = (s * 2 + i // 4) * 1024 + i % 4 * 32
            v = [(back[a, 0, pl.ds(at, 16), :], back[a, 1, pl.ds(at, 16), :]) for a in range(8)]
            for a, y in enumerate(eight(v, -1)):
                for part in range(2):
                    rows_out[pl.ds(start + 128 * a + part, 16, stride=2), :] = y[part]
            return carry

        lax.fori_loop(0, 8, close_eight, 0)

    for s in range(3):
        here(put2.at[s, :, some], got2.at[s, :, some], send2, recv2.at[s]).wait_recv()
        inner(s)
        got3[s, :, me] = put3[s, :, me]
        if s < 2:
            everyone(
                lambda to, device: remote(
                    put3.at[s, :, to], got3.at[s, :, me], send3, recv3.at[s], device
                ).start()
            )
        else:
            for t in range(2):
                everyone(
                    lambda to, device: remote(
                        put3.at[s, t, to], got3.at[s, t, me], send3, recv3.at[s + t], device
                    ).start()
                )

    def outer_backward(s, h):
        columns = []
        for j in range(2):
            s8 = 2 * h + j
            at = (s * 2 + h // 2) * 1024 + (h % 2 * 2 + j) * 2
            z = tuple(rows3[pl.ds(at + part, 128, stride=8), :] for part in range(2))
            z = times_conj(z, (outer_turn[s, s8, 0], outer_turn[s, s8, 1]))
            columns.append(jnp.concatenate(z, axis=0))
        return left(last[s, 0], last[s, 1], jnp.concatenate(columns, axis=1))

    for s in range(2):
        here(put3.at[s, :, some], got3.at[s, :, some], send3, recv3.at[s]).wait_recv()

        def keep(h, carry):
            held[s, h] = outer_backward(s, h)
            return carry

        lax.fori_loop(0, 4, keep, 0)

    own_out = []
    for t in range(2):
        here(put3.at[2, t, some], got3.at[2, t, some], send3, recv3.at[2 + t]).wait_recv()

        def finish(g, carry):
            h = 2 * t + g
            y0, y1, y2 = held[0, h], held[1, h], outer_backward(2, h)
            u, v = y1 + y2, HALF_ROOT3 * (y1 - y2)
            y = y0 - 0.5 * u
            re, im, vr, vi = y[:128], y[128:], v[:128], v[128:]
            for upper, out in enumerate(((re + vi, im - vr), (re - vi, im + vr))):
                for part in range(2):
                    for j in range(2):
                        for e in range(2):
                            at = ((part * 2 + t) * 128 + upper * 64) * 8 + (g * 2 + j) * 2 + e
                            rows4[pl.ds(at, 64, stride=8), :] = out[part][
                                64 * e : 64 * e + 64, 128 * j : 128 * j + 128
                            ]
            return carry

        lax.fori_loop(0, 2, finish, 0)
        own = pltpu.make_async_copy(put4.at[:, t, me], o_ref.at[:, me, t], own_sem.at[1 + t])
        own.start()
        own_out.append(own)
        everyone(
            lambda to, device: remote(
                put4.at[:, t, to], o_ref.at[:, me, t], send4, recv4.at[t], device
            ).start()
        )

    for own in own_out:
        own.wait()
    here(x_ref.at[:, some], got1.at[:, :, some], send1, recv1.at[0]).wait_send()
    for s in range(3):
        here(put2.at[s, :, some], got2.at[s, :, some], send2, recv2.at[s]).wait_send()
        here(put3.at[s, :, some], got3.at[s, :, some], send3, recv3.at[s]).wait_send()
    for t in range(2):
        here(put4.at[:, t, some], o_ref.at[:, some, t], send4, recv4.at[t]).wait()


def hand_over(in_ref, o_ref, sem):
    copy = pltpu.make_async_copy(in_ref, o_ref, sem)
    copy.start()
    copy.wait()


def solution(mesh):
    constants = tables()

    def on_device(modes):
        x = modes.reshape(2, 2, 1024, 128).transpose(0, 2, 1, 3).reshape(2, 128, 2, 8, 128)
        anywhere = pl.BlockSpec(memory_space=pl.ANY)
        dma = pltpu.SemaphoreType.DMA
        out = pl.pallas_call(
            kernel,
            out_shape=pltpu.VMEM((2, 128, 2, 8, 128), F32),
            in_specs=[anywhere] * 5,
            out_specs=pl.BlockSpec(memory_space=pltpu.VMEM),
            scratch_shapes=[
                pltpu.VMEM((3, 2, 256, 256), BF16),
                pltpu.VMEM((3, 2, 256, 256), BF16),
                pltpu.VMEM((2, 2, 256, 256), BF16),
                pltpu.VMEM((6, 2, 128, 128), F32),
                pltpu.VMEM((2, 2, 128, 8, 128), F32),
                pltpu.VMEM((3, 2, 128, 8, 128), F32),
                pltpu.VMEM((3, 2, 128, 8, 128), F32),
                pltpu.VMEM((3, 2, 128, 8, 128), F32),
                pltpu.VMEM((3, 2, 128, 8, 128), F32),
                pltpu.VMEM((2, 2, 128, 8, 128), F32),
                pltpu.VMEM((3, 8, 2, 128, 128), F32),
                pltpu.VMEM((8, 2, 128, 128), F32),
                pltpu.VMEM((8, 2, 128, 128), F32),
                pltpu.VMEM((8, 256, 128), BF16),
                pltpu.VMEM((8, 256, 128), BF16),
                pltpu.VMEM((8, 2, 128, 128), F32),
                pltpu.VMEM((2, 4, 256, 256), F32),
                pltpu.SemaphoreType.REGULAR((3,)),
                dma((4,)),
                dma((3,)),
                dma,
                dma((2,)),
                dma,
                dma((3,)),
                dma,
                dma((4,)),
                dma,
                dma((2,)),
            ],
            compiler_params=pltpu.CompilerParams(
                collective_id=0, has_side_effects=True, vmem_limit_bytes=67043328 - 2**21 - 2**17
            ),
        )(x, *(jnp.asarray(c) for c in constants))
        out = pl.pallas_call(
            hand_over,
            out_shape=jax.ShapeDtypeStruct((2, 128, 2, 8, 128), F32),
            in_specs=[pl.BlockSpec(memory_space=pltpu.VMEM)],
            out_specs=anywhere,
            scratch_shapes=[dma],
            compiler_params=pltpu.CompilerParams(vmem_limit_bytes=2**17),
        )(out)
        return out.reshape(2, 1024, 2, 128).transpose(0, 2, 1, 3).reshape(2, 2, LOCAL)

    spec = P(None, "res", "blk")
    return jax.shard_map(on_device, mesh=mesh, in_specs=(spec,), out_specs=spec, check_vma=False)
```
